32 devices in a mesh: row: 4 (over z), col: 8 (over y, x, core).
Axes of the slice: x: 2, y: 2, z: 4, core: 2. Of those that a mesh axis runs over, the one named last changes fastest.
Arguments:
- node_feats: bfloat16 [4096, 512], P(('row', 'col')), may hold values from -80 to 80
- block_mask: int32 [32, 32], replicated, may hold values from 0 to 1, as said below
- w_qkv: bfloat16 [2, 512, 1536], replicated, may hold values from -0.25 to 0.25
- w_out: bfloat16 [2, 512, 512], replicated, may hold values from -0.79296875 to 0.79296875
- w_up: bfloat16 [2, 512, 1024], replicated, may hold values from -0.25 to 0.25
- w_down: bfloat16 [2, 1024, 512], replicated, may hold values from -0.1875 to 0.1875
- ln_gain: float32 [2, 2, 512], replicated, may hold values from 0.1 to 1.9
- ln_bias: float32 [2, 2, 512], replicated, may hold values from -3 to 3
Outputs:
- nodes_out: bfloat16 [4096, 512], P(('row', 'col'))
The draws below stay inside these ranges and needn't reach their ends.
Inputs may be any that keep to these rules, and one draw needn't show every extreme that they name: `block_mask`: A symmetric 0/1 table over the 32 node blocks; every block is linked with itself.
All inputs are finite; a program needn't handle non-finite values.
Results may differ from the reference program's by a relative error of at most 0.022.
Values may be sent and summed in bfloat16 or wider, within the bound.
A program may use at most 128 MiB of HBM per device.

```python
import jax
import jax.numpy as jnp
from jax import lax

D = 512
HEADS = 8
FF = 1024
BLOCK = 128
LAYERS = 2
NB = 32
NODES = 4096
N_ROW = 4


def draw_node_feats(key, part):
    base = jnp.clip(jax.random.normal(key, (NODES, D), jnp.float32), -6.0, 6.0)
    return base.astype(jnp.bfloat16)


def draw_block_mask(key, part):
    index = jnp.arange(NB, dtype=jnp.int32)
    apart = jnp.abs(index[:, None] - index[None, :])
    apart = jnp.minimum(apart, NB - apart)
    random_bits = jax.random.randint(key, (NB, NB), 0, 16, dtype=jnp.int32)
    busy = jax.random.randint(jax.random.fold_in(key, 1), (NB,), 0, 8, dtype=jnp.int32) == 0
    far_row = NB // 2
    far_col = NB // (2 * N_ROW)
    limit = jnp.where(apart <= 1, 12, jnp.where(apart <= 3, 3, 0))
    limit = jnp.where(busy[:, None] | busy[None, :], jnp.maximum(limit, 2), limit)
    limit = jnp.where((apart == far_row) | (apart == far_col), 16, limit)
    upper = random_bits < limit
    linked = upper | upper.T | (apart == 0)
    return linked.astype(jnp.int32)


def scatter_about(rng, dims, scale, most, kind=jnp.bfloat16):
    array = scale * jax.random.normal(rng, dims, jnp.float32)
    return jnp.clip(array, min=-most, max=most).astype(kind)


def setup_inputs(seed: int = 0) -> dict:
    key_of = jax.random.split(jax.random.key(seed), 9)
    return {
        "node_feats": draw_node_feats(jax.random.fold_in(key_of[8], 71), 0),
        "block_mask": draw_block_mask(jax.random.fold_in(key_of[8], 71), 0),
        "w_qkv": scatter_about(key_of[2], (LAYERS, D, 3 * D), D ** -0.5, 0.25),
        "w_out": scatter_about(key_of[3], (LAYERS, D, D), (3.0 * D ** -0.5), 0.79296875),
        "w_up": scatter_about(key_of[4], (LAYERS, D, FF), D ** -0.5, 0.25),
        "w_down": scatter_about(key_of[5], (LAYERS, FF, D), FF ** -0.5, 0.1875),
        "ln_gain": jnp.clip(1.0 + 0.18 * jax.random.normal(key_of[6], (LAYERS, 2, D), jnp.float32), 0.1, 1.9),
        "ln_bias": scatter_about(key_of[7], (LAYERS, 2, D), 0.5, 3.0, jnp.float32),
    }


def layer_norm(values, gain, bias):
    center = values - lax.optimization_barrier(jnp.mean(values, axis=-1, keepdims=True))
    spread = lax.optimization_barrier(jnp.mean(center * center, axis=-1, keepdims=True))
    return center * lax.rsqrt(spread + 1e-05) * gain + bias

def attend(queries, keys, values, block_mask):
    head_dim = D // HEADS
    qrows = 512
    qsplit = queries.astype(jnp.float32).reshape(NODES // qrows, qrows, HEADS, head_dim)
    ksplit = keys.astype(jnp.float32).reshape(NODES, HEADS, head_dim)
    vsplit = values.astype(jnp.float32).reshape(NODES, HEADS, head_dim)
    mask_rows = block_mask.reshape(NODES // qrows, qrows // BLOCK, NB)

    def one_block(item):
        qblock, mblock = item
        scores = jnp.einsum('qhd,khd->hqk', qblock, ksplit) * (1.0 / head_dim ** 0.5)
        allowed = (jnp.repeat(jnp.repeat(mblock, BLOCK, axis=0), BLOCK, axis=1) > 0)[None]
        peak = lax.optimization_barrier(jnp.max(jnp.where(allowed, scores, -1e+30), axis=-1, keepdims=True))
        weights = jnp.where(allowed, jnp.exp(scores - peak), 0.0)
        mass = lax.optimization_barrier(jnp.sum(weights, axis=-1))
        rounded = lax.optimization_barrier(weights.astype(jnp.bfloat16)).astype(jnp.float32)
        summed = jnp.einsum('hqk,khd->qhd', rounded, vsplit)
        return (summed / mass.T[:, :, None]).reshape(qrows, D).astype(jnp.bfloat16)
    return lax.map(one_block, (qsplit, mask_rows)).reshape(NODES, D)

def reference(node_feats, block_mask, w_qkv, w_out, w_up, w_down, ln_gain, ln_bias):
    x = node_feats
    for layer in range(LAYERS):
        qkv = jnp.dot(x, w_qkv[layer], preferred_element_type=jnp.float32).astype(jnp.bfloat16)
        attn = attend(qkv[:, :D], qkv[:, D:2 * D], qkv[:, 2 * D:], block_mask)
        mixed = jnp.dot(attn, w_out[layer], preferred_element_type=jnp.float32)
        hidden = layer_norm(x.astype(jnp.float32) + mixed, ln_gain[layer, 0], ln_bias[layer, 0]).astype(jnp.bfloat16)
        up = jax.nn.gelu(jnp.dot(hidden, w_up[layer], preferred_element_type=jnp.float32)).astype(jnp.bfloat16)
        down = jnp.dot(up, w_down[layer], preferred_element_type=jnp.float32)
        x = layer_norm(hidden.astype(jnp.float32) + down, ln_gain[layer, 1], ln_bias[layer, 1]).astype(jnp.bfloat16)
    return x
```

```python
import functools

import jax
import jax.numpy as jnp
from jax import lax
from jax.experimental import pallas as pl
from jax.experimental.pallas import tpu as pltpu
from jax.sharding import PartitionSpec as P

HEADS = 8
BLOCK = 128
HALF = HEADS // 2
NEG = -1e30
BIG = 1e30
MESH = pl.DeviceIdType.MESH
F32 = jnp.float32
BF16 = jnp.bfloat16


def bits_of(n):
    return [1 << b for b in range(max(n - 1, 0).bit_length())]


def partner_of(i, k, n):
    out = i
    for b in bits_of(n):
        own = lax.rem(lax.div(i, b), 2)
        flip = (k // b) % 2 if isinstance(k, int) else lax.rem(lax.div(k, b), 2)
        out = out + b * (lax.rem(own + flip, 2) - own)
    return out


def layer_norm(values, gain, bias):
    center = values - jnp.mean(values, axis=-1, keepdims=True)
    spread = jnp.mean(center * center, axis=-1, keepdims=True)
    return center * lax.rsqrt(spread + 1e-05) * gain + bias


def kernel(
    n_row, chips, layers,
    x_ref, mask_ref, wqkv_hbm, wout_hbm, wup_hbm, wdown_hbm, gain_ref, bias_ref,
    out_ref,
    wqkv, wout, wup, wdown, wsem,
    xbuf, xs, qsend, qbuf, rs, st, obuf, sbuf,
    kbuf, vbuf, qpad, acc, top,
    xz_send, xz_recv, xd_send, xd_recv, q_send, q_recv, o_send, o_recv, s_send, s_recv,
):
    rows, width = x_ref.shape
    head_dim = width // HEADS
    hw = width // 2
    n_col = 2 * chips
    z = lax.axis_index("row")
    col = lax.axis_index("col")
    p = lax.div(col, 2)
    c = lax.rem(col, 2)
    mate = 2 * p + 1 - c

    def weight_copies(layer):
        pairs = ((wqkv_hbm, wqkv), (wout_hbm, wout), (wup_hbm, wup), (wdown_hbm, wdown))
        return [
            pltpu.make_async_copy(a.at[layer], b.at[layer], wsem.at[layer, i])
            for i, (a, b) in enumerate(pairs)
        ]

    for layer in range(layers):
        for copy in weight_copies(layer):
            copy.start()

    barrier = pltpu.get_barrier_semaphore()
    for k in range(1, n_row):
        pl.semaphore_signal(
            barrier, inc=1, device_id=(partner_of(z, k, n_row), col), device_id_type=MESH
        )
    pl.semaphore_signal(barrier, inc=1, device_id=(z, mate), device_id_type=MESH)
    for k in range(1, chips):
        for d in range(2):
            pl.semaphore_signal(
                barrier, inc=1, device_id=(z, 2 * partner_of(p, k, chips) + d), device_id_type=MESH
            )
    pl.semaphore_wait(barrier, n_row - 1 + 1 + 2 * (chips - 1))

    def send(src, dst, send_sem, recv_sem, row, column):
        return pltpu.make_async_remote_copy(
            src_ref=src, dst_ref=dst, send_sem=send_sem, recv_sem=recv_sem,
            device_id=(row, column), device_id_type=MESH,
        )

    lane = lax.broadcasted_iota(jnp.int32, (1, 2 * BLOCK), 1)
    ones = jnp.ones((16, 2 * BLOCK), BF16)
    pad = jnp.zeros((head_dim, 2 * BLOCK), BF16)

    for layer in range(layers):
        own_x = x_ref if layer == 0 else xs.at[layer]

        x_copies = [
            send(own_x, xbuf.at[layer, k, c], xz_send.at[layer, k], xz_recv.at[layer, k],
                 partner_of(z, k, n_row), col)
            for k in range(1, n_row)
        ]
        d_copies = [
            send(own_x if k == 0 else xbuf.at[layer, k, c], xbuf.at[layer, k, c],
                 xd_send.at[layer, k], xd_recv.at[layer, k], z, mate)
            for k in range(n_row)
        ]
        d_copies[0].start()
        for copy in x_copies:
            copy.start()
        x = own_x[...]
        xbuf[layer, 0, c] = x

        weight_copies(layer)[0].wait()
        q = jnp.dot(x, wqkv[layer, :, :width], preferred_element_type=F32)
        q = q.astype(BF16).astype(F32) * (1.0 / head_dim**0.5)
        qt = q.T.astype(BF16)
        for d in range(2):
            qsend[layer, d] = qt[d * hw:(d + 1) * hw]
        q_copies = []
        for k in range(1, chips):
            for d in range(2):
                q_copies.append(
                    send(qsend.at[layer, d], qbuf.at[layer, k, c],
                         q_send.at[layer, k, d], q_recv.at[layer, k, c],
                         z, 2 * partner_of(p, k, chips) + d)
                )
        q_copies.append(
            send(qsend.at[layer, 1 - c], qbuf.at[layer, 0, c],
                 q_send.at[layer, 0, 0], q_recv.at[layer, 0, c], z, mate)
        )
        for copy in q_copies[::-1]:
            copy.start()
        qbuf[layer, 0, c] = qsend[layer, c]

        def wait_q(m, j):
            send(qsend.at[layer, 0], qbuf.at[layer, m, j], q_send.at[layer, 0, 0],
                 q_recv.at[layer, m, j], z, mate).wait_recv()

        def o_copy(m, j, half, column):
            return (
                send(rs.at[layer, m, j], obuf.at[layer, m, half],
                     o_send.at[layer, m, j], o_recv.at[layer, m, half], z, column),
                send(st.at[layer, m, j], sbuf.at[layer, m, half],
                     s_send.at[layer, m, j], s_recv.at[layer, m, half], z, column),
            )

        def pair(step, m):
            first, last = step == 0, step == n_row - 1
            if first:
                for h in range(HALF):
                    block = jnp.concatenate(
                        [qbuf[layer, m, j, h * head_dim:(h + 1) * head_dim, :] for j in range(2)],
                        axis=1,
                    )
                    qpad[m, h] = jnp.concatenate(
                        [block, pad] if h % 2 == 0 else [pad, block], axis=0
                    )
            key_row = partner_of(z, step, n_row)
            q_chip = partner_of(p, m, chips)
            allowed = []
            for j in range(2):
                key_id = key_row * n_col + 2 * p + j
                query_id = z * n_col + 2 * q_chip
                near = mask_ref[query_id, key_id]
                far = mask_ref[query_id + 1, key_id]
                allowed.append(jnp.where(lane < BLOCK, near, far) > 0)
            for h in range(HALF):
                group = (h // 2) * 2 * head_dim
                s = jnp.dot(
                    kbuf[:, group:group + 2 * head_dim], qpad[m, h], preferred_element_type=F32
                )
                parts = [s[:BLOCK], s[BLOCK:]]
                peaks = [
                    jnp.where(ok, jnp.max(part, axis=0, keepdims=True), NEG)
                    for ok, part in zip(allowed, parts)
                ]
                peak = jnp.maximum(*peaks)
                if not first:
                    before = top[m, h:h + 1, :]
                    peak = jnp.maximum(peak, before)
                weights = jnp.concatenate(
                    [jnp.exp(part - jnp.where(ok, peak, BIG)) for ok, part in zip(allowed, parts)],
                    axis=0,
                ).astype(BF16)
                total = jnp.dot(vbuf[h], weights, preferred_element_type=F32)
                if not first:
                    total = total + acc[m, h] * jnp.exp(before - peak)
                if last:
                    mass = total[head_dim:head_dim + 1]
                    part = (total[:head_dim] / jnp.maximum(mass, 1e-30)).astype(BF16)
                    for j in range(2):
                        cut = slice(j * BLOCK, (j + 1) * BLOCK)
                        rs[layer, m, j, h * head_dim:(h + 1) * head_dim, :] = part[:, cut]
                        st[layer, m, j, h:h + 1, :] = peak[:, cut]
                        st[layer, m, j, HALF + h:HALF + h + 1, :] = mass[:, cut]
                else:
                    acc[m, h] = total
                    top[m, h:h + 1, :] = peak

        for step in range(n_row):
            if step > 0:
                x_copies[step - 1].wait_recv()
                d_copies[step].start()
            d_copies[step].wait_recv()
            chunk = xbuf[layer, step].reshape(2 * rows, width)
            k_cols = pl.ds(pl.multiple_of(width + c * hw, hw), hw)
            v_cols = pl.ds(pl.multiple_of(2 * width + c * hw, hw), hw)
            kbuf[...] = jnp.dot(
                chunk, wqkv[layer, :, k_cols], preferred_element_type=F32
            ).astype(BF16)
            vt = jnp.dot(chunk, wqkv[layer, :, v_cols], preferred_element_type=F32).T.astype(BF16)
            for h in range(HALF):
                vbuf[h] = jnp.concatenate([vt[h * head_dim:(h + 1) * head_dim], ones], axis=0)
            if step == 0:
                wait_q(0, 1 - c)
                pair(step, 0)

            def body(i, carry, step=step):
                m = i + 1 if step < n_row - 1 else chips - 1 - i
                if step == 0:
                    wait_q(m, 0)
                    wait_q(m, 1)
                pair(step, m)
                if step == n_row - 1:
                    for j in range(2):
                        for copy in o_copy(m, j, c, 2 * partner_of(p, m, chips) + j):
                            copy.start()
                return carry

            lax.fori_loop(0, chips - 1, body, 0)
            if step > 0:
                pair(step, 0)
        for copy in o_copy(0, 1 - c, c, mate):
            copy.start()
        obuf[layer, 0, c] = rs[layer, 0, c]
        sbuf[layer, 0, c] = st[layer, 0, c]

        for copy in weight_copies(layer)[1:]:
            copy.wait()
        for m in range(chips):
            for half in range(2):
                if m > 0:
                    for copy in o_copy(m, half, half, mate):
                        copy.wait_recv()
        for copy in o_copy(0, 1 - c, 1 - c, mate):
            copy.wait_recv()
        heads = []
        for half in range(2):
            for h in range(HALF):
                tops = [sbuf[layer, m, half, h:h + 1, :] for m in range(chips)]
                peak = functools.reduce(jnp.maximum, tops)
                scale = [
                    sbuf[layer, m, half, HALF + h:HALF + h + 1, :] * jnp.exp(tops[m] - peak)
                    for m in range(chips)
                ]
                inverse = 1.0 / functools.reduce(jnp.add, scale)
                cut = slice(h * head_dim, (h + 1) * head_dim)
                heads.append(
                    functools.reduce(
                        jnp.add,
                        [
                            obuf[layer, m, half, cut, :].astype(F32) * (scale[m] * inverse)
                            for m in range(chips)
                        ],
                    )
                )
        attn = jnp.concatenate(heads, axis=0).T.astype(BF16)

        mixed = jnp.dot(attn, wout[layer], preferred_element_type=F32)
        hidden = layer_norm(
            x.astype(F32) + mixed, gain_ref[layer, 0:1, :], bias_ref[layer, 0:1, :]
        ).astype(BF16)
        up = jax.nn.gelu(jnp.dot(hidden, wup[layer], preferred_element_type=F32)).astype(BF16)
        down = jnp.dot(up, wdown[layer], preferred_element_type=F32)
        result = layer_norm(
            hidden.astype(F32) + down, gain_ref[layer, 1:2, :], bias_ref[layer, 1:2, :]
        ).astype(BF16)
        if layer == layers - 1:
            out_ref[...] = result
        else:
            xs[layer + 1] = result

        for copy in x_copies + d_copies + q_copies:
            copy.wait_send()
        for m in range(chips):
            for j in range(2):
                if m > 0:
                    for copy in o_copy(m, j, c, mate):
                        copy.wait_send()
        for copy in o_copy(0, 1 - c, c, mate):
            copy.wait_send()


def per_device(n_row, n_col, node_feats, block_mask, w_qkv, w_out, w_up, w_down, ln_gain, ln_bias):
    rows, width = node_feats.shape
    layers = w_qkv.shape[0]
    chips = n_col // 2
    assert rows == BLOCK
    hw = width // 2
    head_dim = width // HEADS
    vmem = pl.BlockSpec(memory_space=pltpu.VMEM)
    hbm = pl.BlockSpec(memory_space=pl.ANY)
    dma = pltpu.SemaphoreType.DMA
    return pl.pallas_call(
        functools.partial(kernel, n_row, chips, layers),
        out_shape=jax.ShapeDtypeStruct((rows, width), BF16),
        in_specs=[vmem, pl.BlockSpec(memory_space=pltpu.SMEM), hbm, hbm, hbm, hbm, vmem, vmem],
        out_specs=vmem,
        scratch_shapes=[
            pltpu.VMEM(w_qkv.shape, BF16),
            pltpu.VMEM(w_out.shape, BF16),
            pltpu.VMEM(w_up.shape, BF16),
            pltpu.VMEM(w_down.shape, BF16),
            dma((layers, 4)),
            pltpu.VMEM((layers, n_row, 2, rows, width), BF16),
            pltpu.VMEM((layers, rows, width), BF16),
            pltpu.VMEM((layers, 2, hw, rows), BF16),
            pltpu.VMEM((layers, chips, 2, hw, rows), BF16),
            pltpu.VMEM((layers, chips, 2, hw, rows), BF16),
            pltpu.VMEM((layers, chips, 2, HEADS, rows), F32),
            pltpu.VMEM((layers, chips, 2, hw, rows), BF16),
            pltpu.VMEM((layers, chips, 2, HEADS, rows), F32),
            pltpu.VMEM((2 * rows, hw), BF16),
            pltpu.VMEM((HALF, head_dim + 16, 2 * rows), BF16),
            pltpu.VMEM((chips, HALF, 2 * head_dim, 2 * rows), BF16),
            pltpu.VMEM((chips, HALF, head_dim + 16, 2 * rows), F32),
            pltpu.VMEM((chips, HEADS, 2 * rows), F32),
            dma((layers, n_row)),
            dma((layers, n_row)),
            dma((layers, n_row)),
            dma((layers, n_row)),
            dma((layers, chips, 2)),
            dma((layers, chips, 2)),
            dma((layers, chips, 2)),
            dma((layers, chips, 2)),
            dma((layers, chips, 2)),
            dma((layers, chips, 2)),
        ],
        compiler_params=pltpu.CompilerParams(
            collective_id=0, has_side_effects=True, vmem_limit_bytes=56 * 1024 * 1024
        ),
    )(node_feats, block_mask, w_qkv, w_out, w_up, w_down, ln_gain, ln_bias)


def solution(mesh):
    placed = (P(("row", "col"), None), P(), P(), P(), P(), P(), P(), P())
    body = functools.partial(per_device, mesh.shape["row"], mesh.shape["col"])
    return jax.shard_map(
        body, mesh=mesh, in_specs=placed, out_specs=P(("row", "col"), None), check_vma=False
    )
```

```python
import functools

import jax
import jax.numpy as jnp
from jax import lax
from jax.experimental import pallas as pl
from jax.experimental.pallas import tpu as pltpu
from jax.sharding import PartitionSpec as P

HEADS = 8
BLOCK = 128
HALF = HEADS // 2
KEEP = 1
NEG = -1e30
BIG = 1e30
MESH = pl.DeviceIdType.MESH
F32 = jnp.float32
BF16 = jnp.bfloat16


def bits_of(n):
    return [1 << b for b in range(max(n - 1, 0).bit_length())]


def partner_of(i, k, n):
    out = i
    for b in bits_of(n):
        own = lax.rem(lax.div(i, b), 2)
        flip = (k // b) % 2 if isinstance(k, int) else lax.rem(lax.div(k, b), 2)
        out = out + b * (lax.rem(own + flip, 2) - own)
    return out


def layer_norm(values, gain, bias):
    center = values - jnp.mean(values, axis=-1, keepdims=True)
    spread = jnp.mean(center * center, axis=-1, keepdims=True)
    return center * lax.rsqrt(spread + 1e-05) * gain + bias


def kernel(
    n_row, chips, layers,
    x_ref, mask_ref, wqkv_hbm, wout_hbm, wup_hbm, wdown_hbm, gain_ref, bias_ref,
    out_ref,
    wqkv, wout, wup, wdown, wsem,
    xbuf, xs, qsend, qbuf, rs, st, obuf, sbuf,
    kbuf, vbuf, qpad, acc, top,
    xz_send, xz_recv, xd_send, xd_recv, q_send, q_recv, o_send, o_recv, s_send, s_recv,
):
    rows, width = x_ref.shape
    head_dim = width // HEADS
    hw = width // 2
    n_col = 2 * chips
    z = lax.axis_index("row")
    col = lax.axis_index("col")
    p = lax.div(col, 2)
    c = lax.rem(col, 2)
    mate = 2 * p + 1 - c

    def weight_copies(layer):
        pairs = ((wqkv_hbm, wqkv), (wout_hbm, wout), (wup_hbm, wup), (wdown_hbm, wdown))
        return [
            pltpu.make_async_copy(a.at[layer], b.at[layer], wsem.at[layer, i])
            for i, (a, b) in enumerate(pairs)
        ]

    for layer in range(layers):
        for copy in weight_copies(layer):
            copy.start()

    barrier = pltpu.get_barrier_semaphore()
    for k in range(1, n_row):
        pl.semaphore_signal(
            barrier, inc=1, device_id=(partner_of(z, k, n_row), col), device_id_type=MESH
        )
    pl.semaphore_signal(barrier, inc=1, device_id=(z, mate), device_id_type=MESH)
    for k in range(1, chips):
        for d in range(2):
            pl.semaphore_signal(
                barrier, inc=1, device_id=(z, 2 * partner_of(p, k, chips) + d), device_id_type=MESH
            )
    pl.semaphore_wait(barrier, n_row - 1 + 1 + 2 * (chips - 1))

    def send(src, dst, send_sem, recv_sem, row, column):
        return pltpu.make_async_remote_copy(
            src_ref=src, dst_ref=dst, send_sem=send_sem, recv_sem=recv_sem,
            device_id=(row, column), device_id_type=MESH,
        )

    order = list(range(n_row))

    lane = lax.broadcasted_iota(jnp.int32, (1, 2 * BLOCK), 1)
    ones = jnp.ones((16, 2 * BLOCK), BF16)
    pad = jnp.zeros((head_dim, 2 * BLOCK), BF16)

    for layer in range(layers):
        own_x = x_ref if layer == 0 else xs.at[layer]

        x_copies = {
            k: send(own_x, xbuf.at[layer, k, c], xz_send.at[layer, k], xz_recv.at[layer, k],
                    partner_of(z, k, n_row), col)
            for k in order[1:]
        }
        d_copies = [
            send(own_x if k == 0 else xbuf.at[layer, k, c], xbuf.at[layer, k, c],
                 xd_send.at[layer, k], xd_recv.at[layer, k], z, mate)
            for k in range(n_row)
        ]
        d_copies[0].start()
        for k in order[1:]:
            x_copies[k].start()
        x = own_x[...]
        xbuf[layer, 0, c] = x

        weight_copies(layer)[0].wait()
        q = jnp.dot(x, wqkv[layer, :, :width], preferred_element_type=F32)
        q = q.astype(BF16).astype(F32) * (1.0 / head_dim**0.5)
        qt = q.T.astype(BF16)
        for d in range(2):
            qsend[layer, d] = qt[d * hw:(d + 1) * hw]
        q_copies = []
        for k in range(1, chips):
            for d in range(2):
                q_copies.append(
                    send(qsend.at[layer, d], qbuf.at[layer, k, c],
                         q_send.at[layer, k, d], q_recv.at[layer, k, c],
                         z, 2 * partner_of(p, k, chips) + d)
                )
        q_copies.append(
            send(qsend.at[layer, 1 - c], qbuf.at[layer, 0, c],
                 q_send.at[layer, 0, 0], q_recv.at[layer, 0, c], z, mate)
        )
        for copy in q_copies[::-1]:
            copy.start()
        qbuf[layer, 0, c] = qsend[layer, c]

        def wait_q(m, j):
            send(qsend.at[layer, 0], qbuf.at[layer, m, j], q_send.at[layer, 0, 0],
                 q_recv.at[layer, m, j], z, mate).wait_recv()

        def o_copy(m, j, half, column):
            return (
                send(rs.at[layer, m, j], obuf.at[layer, m, half],
                     o_send.at[layer, m, j], o_recv.at[layer, m, half], z, column),
                send(st.at[layer, m, j], sbuf.at[layer, m, half],
                     s_send.at[layer, m, j], s_recv.at[layer, m, half], z, column),
            )

        def pair(step, m):
            first, last = step == order[0], step == order[-1]
            if first:
                for h in range(HALF):
                    block = jnp.concatenate(
                        [qbuf[layer, m, j, h * head_dim:(h + 1) * head_dim, :] for j in range(2)],
                        axis=1,
                    )
                    qpad[m, h] = jnp.concatenate(
                        [block, pad] if h % 2 == 0 else [pad, block], axis=0
                    )
            key_row = partner_of(z, step, n_row)
            q_chip = partner_of(p, m, chips)
            allowed = []
            for j in range(2):
                key_id = key_row * n_col + 2 * p + j
                query_id = z * n_col + 2 * q_chip
                near = mask_ref[query_id, key_id]
                far = mask_ref[query_id + 1, key_id]
                allowed.append(jnp.where(lane < BLOCK, near, far) > 0)
            scores, peaks, before = [], [], []
            for h in range(HALF):
                group = (h // 2) * 2 * head_dim
                scores.append(jnp.dot(
                    kbuf[:, group:group + 2 * head_dim], qpad[m, h], preferred_element_type=F32
                ))
            weights = []
            for h in range(HALF):
                parts = [scores[h][:BLOCK], scores[h][BLOCK:]]
                peak = jnp.maximum(*[
                    jnp.where(ok, jnp.max(part, axis=0, keepdims=True), NEG)
                    for ok, part in zip(allowed, parts)
                ])
                if not first:
                    before.append(top[m, h:h + 1, :])
                    peak = jnp.maximum(peak, before[h])
                peaks.append(peak)
                weights.append(jnp.concatenate(
                    [jnp.exp(part - jnp.where(ok, peak, BIG)) for ok, part in zip(allowed, parts)],
                    axis=0,
                ).astype(BF16))
            totals = [
                jnp.dot(vbuf[h], weights[h], preferred_element_type=F32) for h in range(HALF)
            ]
            for h in range(HALF):
                total, peak = totals[h], peaks[h]
                if not first:
                    total = total + acc[m, h] * jnp.exp(before[h] - peak)
                if last:
                    mass = total[head_dim:head_dim + 1]
                    part = (total[:head_dim] / jnp.maximum(mass, 1e-30)).astype(BF16)
                    for j in range(2):
                        cut = slice(j * BLOCK, (j + 1) * BLOCK)
                        rs[layer, m, j, h * head_dim:(h + 1) * head_dim, :] = part[:, cut]
                        st[layer, m, j, h:h + 1, :] = peak[:, cut]
                        st[layer, m, j, HALF + h:HALF + h + 1, :] = mass[:, cut]
                else:
                    acc[m, h] = total
                    top[m, h:h + 1, :] = peak

        def pass_on(step):
            x_copies[step].wait_recv()
            d_copies[step].start()

        for turn, step in enumerate(order):
            final = turn == n_row - 1
            d_copies[step].wait_recv()
            chunk = xbuf[layer, step].reshape(2 * rows, width)
            k_cols = pl.ds(pl.multiple_of(width + c * hw, hw), hw)
            v_cols = pl.ds(pl.multiple_of(2 * width + c * hw, hw), hw)
            kbuf[...] = jnp.dot(
                chunk, wqkv[layer, :, k_cols], preferred_element_type=F32
            ).astype(BF16)
            vt = jnp.dot(chunk, wqkv[layer, :, v_cols], preferred_element_type=F32).T.astype(BF16)
            for h in range(HALF):
                vbuf[h] = jnp.concatenate([vt[h * head_dim:(h + 1) * head_dim], ones], axis=0)
            if turn == 0:
                wait_q(0, 1 - c)
                pair(step, 0)

            def body(i, carry, turn=turn, step=step, final=final):
                m = chips - 1 - i if final else i + 1
                if turn == 0:
                    wait_q(m, 0)
                    wait_q(m, 1)
                pair(step, m)
                if final:
                    for j in range(2):
                        for copy in o_copy(m, j, c, 2 * partner_of(p, m, chips) + j):
                            copy.start()
                return carry

            early = chips - 1 if final else max(chips - 1 - KEEP, 0)
            lax.fori_loop(0, early, body, 0)
            if not final:
                pass_on(order[turn + 1])
                lax.fori_loop(early, chips - 1, body, 0)
            if turn > 0:
                pair(step, 0)
        for copy in o_copy(0, 1 - c, c, mate):
            copy.start()
        obuf[layer, 0, c] = rs[layer, 0, c]
        sbuf[layer, 0, c] = st[layer, 0, c]

        for copy in weight_copies(layer)[1:]:
            copy.wait()
        for m in range(chips):
            for half in range(2):
                if m > 0:
                    for copy in o_copy(m, half, half, mate):
                        copy.wait_recv()
        for copy in o_copy(0, 1 - c, 1 - c, mate):
            copy.wait_recv()
        heads = []
        for half in range(2):
            for h in range(HALF):
                tops = [sbuf[layer, m, half, h:h + 1, :] for m in range(chips)]
                peak = functools.reduce(jnp.maximum, tops)
                scale = [
                    sbuf[layer, m, half, HALF + h:HALF + h + 1, :] * jnp.exp(tops[m] - peak)
                    for m in range(chips)
                ]
                inverse = 1.0 / functools.reduce(jnp.add, scale)
                cut = slice(h * head_dim, (h + 1) * head_dim)
                heads.append(
                    functools.reduce(
                        jnp.add,
                        [
                            obuf[layer, m, half, cut, :].astype(F32) * (scale[m] * inverse)
                            for m in range(chips)
                        ],
                    )
                )
        attn = jnp.concatenate(heads, axis=0).T.astype(BF16)

        mixed = jnp.dot(attn, wout[layer], preferred_element_type=F32)
        hidden = layer_norm(
            x.astype(F32) + mixed, gain_ref[layer, 0:1, :], bias_ref[layer, 0:1, :]
        ).astype(BF16)
        up = jax.nn.gelu(jnp.dot(hidden, wup[layer], preferred_element_type=F32)).astype(BF16)
        down = jnp.dot(up, wdown[layer], preferred_element_type=F32)
        result = layer_norm(
            hidden.astype(F32) + down, gain_ref[layer, 1:2, :], bias_ref[layer, 1:2, :]
        ).astype(BF16)
        if layer == layers - 1:
            out_ref[...] = result
        else:
            xs[layer + 1] = result

        for k in order[1:]:
            x_copies[k].wait_send()
        for copy in d_copies + q_copies:
            copy.wait_send()
        for m in range(chips):
            for j in range(2):
                if m > 0:
                    for copy in o_copy(m, j, c, mate):
                        copy.wait_send()
        for copy in o_copy(0, 1 - c, c, mate):
            copy.wait_send()


def per_device(n_row, n_col, node_feats, block_mask, w_qkv, w_out, w_up, w_down, ln_gain, ln_bias):
    rows, width = node_feats.shape
    layers = w_qkv.shape[0]
    chips = n_col // 2
    assert rows == BLOCK
    hw = width // 2
    head_dim = width // HEADS
    vmem = pl.BlockSpec(memory_space=pltpu.VMEM)
    hbm = pl.BlockSpec(memory_space=pl.ANY)
    dma = pltpu.SemaphoreType.DMA
    return pl.pallas_call(
        functools.partial(kernel, n_row, chips, layers),
        out_shape=jax.ShapeDtypeStruct((rows, width), BF16),
        in_specs=[vmem, pl.BlockSpec(memory_space=pltpu.SMEM), hbm, hbm, hbm, hbm, vmem, vmem],
        out_specs=vmem,
        scratch_shapes=[
            pltpu.VMEM(w_qkv.shape, BF16),
            pltpu.VMEM(w_out.shape, BF16),
            pltpu.VMEM(w_up.shape, BF16),
            pltpu.VMEM(w_down.shape, BF16),
            dma((layers, 4)),
            pltpu.VMEM((layers, n_row, 2, rows, width), BF16),
            pltpu.VMEM((layers, rows, width), BF16),
            pltpu.VMEM((layers, 2, hw, rows), BF16),
            pltpu.VMEM((layers, chips, 2, hw, rows), BF16),
            pltpu.VMEM((layers, chips, 2, hw, rows), BF16),
            pltpu.VMEM((layers, chips, 2, HEADS, rows), F32),
            pltpu.VMEM((layers, chips, 2, hw, rows), BF16),
            pltpu.VMEM((layers, chips, 2, HEADS, rows), F32),
            pltpu.VMEM((2 * rows, hw), BF16),
            pltpu.VMEM((HALF, head_dim + 16, 2 * rows), BF16),
            pltpu.VMEM((chips, HALF, 2 * head_dim, 2 * rows), BF16),
            pltpu.VMEM((chips, HALF, head_dim + 16, 2 * rows), F32),
            pltpu.VMEM((chips, HEADS, 2 * rows), F32),
            dma((layers, n_row)),
            dma((layers, n_row)),
            dma((layers, n_row)),
            dma((layers, n_row)),
            dma((layers, chips, 2)),
            dma((layers, chips, 2)),
            dma((layers, chips, 2)),
            dma((layers, chips, 2)),
            dma((layers, chips, 2)),
            dma((layers, chips, 2)),
        ],
        compiler_params=pltpu.CompilerParams(
            collective_id=0, has_side_effects=True, vmem_limit_bytes=56 * 1024 * 1024
        ),
    )(node_feats, block_mask, w_qkv, w_out, w_up, w_down, ln_gain, ln_bias)


def solution(mesh):
    placed = (P(("row", "col"), None), P(), P(), P(), P(), P(), P(), P())
    body = functools.partial(per_device, mesh.shape["row"], mesh.shape["col"])
    return jax.shard_map(
        body, mesh=mesh, in_specs=placed, out_specs=P(("row", "col"), None), check_vma=False
    )
```

```python
import functools

import jax
import jax.numpy as jnp
from jax import lax
from jax.experimental import pallas as pl
from jax.experimental.pallas import tpu as pltpu
from jax.sharding import PartitionSpec as P

HEADS = 8
BLOCK = 128
HALF = HEADS // 2
KEEP = 1
NEG = -1e30
BIG = 1e30
MESH = pl.DeviceIdType.MESH
F32 = jnp.float32
BF16 = jnp.bfloat16


def bits_of(n):
    return [1 << b for b in range(max(n - 1, 0).bit_length())]


def partner_of(i, k, n):
    out = i
    for b in bits_of(n):
        own = lax.rem(lax.div(i, b), 2)
        flip = (k // b) % 2 if isinstance(k, int) else lax.rem(lax.div(k, b), 2)
        out = out + b * (lax.rem(own + flip, 2) - own)
    return out


def layer_norm(values, gain, bias):
    center = values - jnp.mean(values, axis=-1, keepdims=True)
    spread = jnp.mean(center * center, axis=-1, keepdims=True)
    return center * lax.rsqrt(spread + 1e-05) * gain + bias


def kernel(
    n_row, chips, layers,
    x_ref, mask_ref, wqkv_hbm, wout_hbm, wup_hbm, wdown_hbm, gain_ref, bias_ref,
    out_ref,
    wqkv, wout, wup, wdown, wsem,
    xbuf, xs, qsend, qbuf, rs, st, obuf, sbuf,
    kbuf, vbuf, qpad, acc, top,
    xz_send, xz_recv, xd_send, xd_recv, q_send, q_recv, o_send, o_recv, s_send, s_recv,
):
    rows, width = x_ref.shape
    head_dim = width // HEADS
    hw = width // 2
    n_col = 2 * chips
    z = lax.axis_index("row")
    col = lax.axis_index("col")
    p = lax.div(col, 2)
    c = lax.rem(col, 2)
    mate = 2 * p + 1 - c

    def weight_copies(layer):
        pairs = ((wqkv_hbm, wqkv), (wout_hbm, wout), (wup_hbm, wup), (wdown_hbm, wdown))
        return [
            pltpu.make_async_copy(a.at[layer], b.at[layer], wsem.at[layer, i])
            for i, (a, b) in enumerate(pairs)
        ]

    for layer in range(layers):
        for copy in weight_copies(layer):
            copy.start()

    barrier = pltpu.get_barrier_semaphore()
    for k in range(1, n_row):
        pl.semaphore_signal(
            barrier, inc=1, device_id=(partner_of(z, k, n_row), col), device_id_type=MESH
        )
    pl.semaphore_signal(barrier, inc=1, device_id=(z, mate), device_id_type=MESH)
    for k in range(1, chips):
        for d in range(2):
            pl.semaphore_signal(
                barrier, inc=1, device_id=(z, 2 * partner_of(p, k, chips) + d), device_id_type=MESH
            )
    pl.semaphore_wait(barrier, n_row - 1 + 1 + 2 * (chips - 1))

    def send(src, dst, send_sem, recv_sem, row, column):
        return pltpu.make_async_remote_copy(
            src_ref=src, dst_ref=dst, send_sem=send_sem, recv_sem=recv_sem,
            device_id=(row, column), device_id_type=MESH,
        )

    order = list(range(n_row))

    lane = lax.broadcasted_iota(jnp.int32, (1, 2 * BLOCK), 1)
    ones = jnp.ones((16, 2 * BLOCK), BF16)
    pad = jnp.zeros((head_dim, 2 * BLOCK), BF16)

    for layer in range(layers):
        own_x = x_ref if layer == 0 else xs.at[layer]

        x_copies = {
            k: send(own_x, xbuf.at[layer, k, c], xz_send.at[layer, k], xz_recv.at[layer, k],
                    partner_of(z, k, n_row), col)
            for k in order[1:]
        }
        d_copies = [
            send(own_x if k == 0 else xbuf.at[layer, k, c], xbuf.at[layer, k, c],
                 xd_send.at[layer, k], xd_recv.at[layer, k], z, mate)
            for k in range(n_row)
        ]
        d_copies[0].start()
        for k in order[1:]:
            x_copies[k].start()
        x = own_x[...]
        xbuf[layer, 0, c] = x

        weight_copies(layer)[0].wait()
        q = jnp.dot(x, wqkv[layer, :, :width], preferred_element_type=F32)
        q = q.astype(BF16).astype(F32) * (1.0 / head_dim**0.5)
        qt = q.T.astype(BF16)
        for d in range(2):
            qsend[layer, d] = qt[d * hw:(d + 1) * hw]
        q_copies = []
        for k in range(1, chips):
            for d in range(2):
                q_copies.append(
                    send(qsend.at[layer, d], qbuf.at[layer, k, c],
                         q_send.at[layer, k, d], q_recv.at[layer, k, c],
                         z, 2 * partner_of(p, k, chips) + d)
                )
        q_copies.append(
            send(qsend.at[layer, 1 - c], qbuf.at[layer, 0, c],
                 q_send.at[layer, 0, 0], q_recv.at[layer, 0, c], z, mate)
        )
        for copy in q_copies[-1:] + q_copies[:-1]:
            copy.start()
        qbuf[layer, 0, c] = qsend[layer, c]

        def wait_q(m, j):
            send(qsend.at[layer, 0], qbuf.at[layer, m, j], q_send.at[layer, 0, 0],
                 q_recv.at[layer, m, j], z, mate).wait_recv()

        def o_copy(m, j, half, column):
            return (
                send(rs.at[layer, m, j], obuf.at[layer, m, half],
                     o_send.at[layer, m, j], o_recv.at[layer, m, half], z, column),
                send(st.at[layer, m, j], sbuf.at[layer, m, half],
                     s_send.at[layer, m, j], s_recv.at[layer, m, half], z, column),
            )

        def pair(step, m):
            first, last = step == order[0], step == order[-1]
            if first:
                for h in range(HALF):
                    block = jnp.concatenate(
                        [qbuf[layer, m, j, h * head_dim:(h + 1) * head_dim, :] for j in range(2)],
                        axis=1,
                    )
                    qpad[m, h] = jnp.concatenate(
                        [block, pad] if h % 2 == 0 else [pad, block], axis=0
                    )
            key_row = partner_of(z, step, n_row)
            q_chip = partner_of(p, m, chips)
            allowed = []
            for j in range(2):
                key_id = key_row * n_col + 2 * p + j
                query_id = z * n_col + 2 * q_chip
                near = mask_ref[query_id, key_id]
                far = mask_ref[query_id + 1, key_id]
                allowed.append(jnp.where(lane < BLOCK, near, far) > 0)
            scores, peaks, before = [], [], []
            for h in range(HALF):
                group = (h // 2) * 2 * head_dim
                scores.append(jnp.dot(
                    kbuf[step, :, group:group + 2 * head_dim], qpad[m, h], preferred_element_type=F32
                ))
            weights = []
            for h in range(HALF):
                parts = [scores[h][:BLOCK], scores[h][BLOCK:]]
                peak = jnp.maximum(*[
                    jnp.where(ok, jnp.max(part, axis=0, keepdims=True), NEG)
                    for ok, part in zip(allowed, parts)
                ])
                if not first:
                    before.append(top[m, h:h + 1, :])
                    peak = jnp.maximum(peak, before[h])
                peaks.append(peak)
                weights.append(jnp.concatenate(
                    [jnp.exp(part - jnp.where(ok, peak, BIG)) for ok, part in zip(allowed, parts)],
                    axis=0,
                ).astype(BF16))
            totals = [
                jnp.dot(vbuf[step, h], weights[h], preferred_element_type=F32) for h in range(HALF)
            ]
            for h in range(HALF):
                total, peak = totals[h], peaks[h]
                if not first:
                    total = total + acc[m, h] * jnp.exp(before[h] - peak)
                if last:
                    mass = total[head_dim:head_dim + 1]
                    part = (total[:head_dim] / jnp.maximum(mass, 1e-30)).astype(BF16)
                    for j in range(2):
                        cut = slice(j * BLOCK, (j + 1) * BLOCK)
                        rs[layer, m, j, h * head_dim:(h + 1) * head_dim, :] = part[:, cut]
                        st[layer, m, j, h:h + 1, :] = peak[:, cut]
                        st[layer, m, j, HALF + h:HALF + h + 1, :] = mass[:, cut]
                else:
                    acc[m, h] = total
                    top[m, h:h + 1, :] = peak

        def pass_on(step):
            x_copies[step].wait_recv()
            d_copies[step].start()

        def project(step):
            chunk = xbuf[layer, step].reshape(2 * rows, width)
            k_cols = pl.ds(pl.multiple_of(width + c * hw, hw), hw)
            v_cols = pl.ds(pl.multiple_of(2 * width + c * hw, hw), hw)
            kbuf[step] = jnp.dot(
                chunk, wqkv[layer, :, k_cols], preferred_element_type=F32
            ).astype(BF16)
            vt = jnp.dot(chunk, wqkv[layer, :, v_cols], preferred_element_type=F32).T.astype(BF16)
            for h in range(HALF):
                vbuf[step, h] = jnp.concatenate(
                    [vt[h * head_dim:(h + 1) * head_dim], ones], axis=0
                )

        d_copies[order[0]].wait_recv()
        project(order[0])
        wait_q(0, 1 - c)
        pair(order[0], 0)
        groups = [order[:2]] + [[step] for step in order[2:]]
        pass_on(order[1])
        for turn, group in enumerate(groups):
            final = turn == len(groups) - 1
            d_copies[group[-1]].wait_recv()
            project(group[-1])
            if turn == 0:
                pair(group[-1], 0)

            def body(i, carry, turn=turn, group=group, final=final):
                m = chips - 1 - i if final else i + 1
                if turn == 0:
                    wait_q(m, 0)
                    wait_q(m, 1)
                for step in group:
                    pair(step, m)
                if final:
                    for j in range(2):
                        for copy in o_copy(m, j, c, 2 * partner_of(p, m, chips) + j):
                            copy.start()
                return carry

            early = chips - 1 if final else max(chips - 1 - KEEP, 0)
            lax.fori_loop(0, early, body, 0)
            if not final:
                pass_on(groups[turn + 1][0])
                lax.fori_loop(early, chips - 1, body, 0)
            if turn > 0:
                pair(group[0], 0)
        for copy in o_copy(0, 1 - c, c, mate):
            copy.start()
        obuf[layer, 0, c] = rs[layer, 0, c]
        sbuf[layer, 0, c] = st[layer, 0, c]

        for copy in weight_copies(layer)[1:]:
            copy.wait()
        for m in range(chips):
            for half in range(2):
                if m > 0:
                    for copy in o_copy(m, half, half, mate):
                        copy.wait_recv()
        for copy in o_copy(0, 1 - c, 1 - c, mate):
            copy.wait_recv()
        heads = []
        for half in range(2):
            for h in range(HALF):
                tops = [sbuf[layer, m, half, h:h + 1, :] for m in range(chips)]
                peak = functools.reduce(jnp.maximum, tops)
                scale = [
                    sbuf[layer, m, half, HALF + h:HALF + h + 1, :] * jnp.exp(tops[m] - peak)
                    for m in range(chips)
                ]
                inverse = 1.0 / functools.reduce(jnp.add, scale)
                cut = slice(h * head_dim, (h + 1) * head_dim)
                heads.append(
                    functools.reduce(
                        jnp.add,
                        [
                            obuf[layer, m, half, cut, :].astype(F32) * (scale[m] * inverse)
                            for m in range(chips)
                        ],
                    )
                )
        attn = jnp.concatenate(heads, axis=0).T.astype(BF16)

        mixed = jnp.dot(attn, wout[layer], preferred_element_type=F32)
        hidden = layer_norm(
            x.astype(F32) + mixed, gain_ref[layer, 0:1, :], bias_ref[layer, 0:1, :]
        ).astype(BF16)
        up = jax.nn.gelu(jnp.dot(hidden, wup[layer], preferred_element_type=F32)).astype(BF16)
        down = jnp.dot(up, wdown[layer], preferred_element_type=F32)
        result = layer_norm(
            hidden.astype(F32) + down, gain_ref[layer, 1:2, :], bias_ref[layer, 1:2, :]
        ).astype(BF16)
        if layer == layers - 1:
            out_ref[...] = result
        else:
            xs[layer + 1] = result

        for k in order[1:]:
            x_copies[k].wait_send()
        for copy in d_copies + q_copies:
            copy.wait_send()
        for m in range(chips):
            for j in range(2):
                if m > 0:
                    for copy in o_copy(m, j, c, mate):
                        copy.wait_send()
        for copy in o_copy(0, 1 - c, c, mate):
            copy.wait_send()


def per_device(n_row, n_col, node_feats, block_mask, w_qkv, w_out, w_up, w_down, ln_gain, ln_bias):
    rows, width = node_feats.shape
    layers = w_qkv.shape[0]
    chips = n_col // 2
    assert rows == BLOCK
    hw = width // 2
    head_dim = width // HEADS
    vmem = pl.BlockSpec(memory_space=pltpu.VMEM)
    hbm = pl.BlockSpec(memory_space=pl.ANY)
    dma = pltpu.SemaphoreType.DMA
    return pl.pallas_call(
        functools.partial(kernel, n_row, chips, layers),
        out_shape=jax.ShapeDtypeStruct((rows, width), BF16),
        in_specs=[vmem, pl.BlockSpec(memory_space=pltpu.SMEM), hbm, hbm, hbm, hbm, vmem, vmem],
        out_specs=vmem,
        scratch_shapes=[
            pltpu.VMEM(w_qkv.shape, BF16),
            pltpu.VMEM(w_out.shape, BF16),
            pltpu.VMEM(w_up.shape, BF16),
            pltpu.VMEM(w_down.shape, BF16),
            dma((layers, 4)),
            pltpu.VMEM((layers, n_row, 2, rows, width), BF16),
            pltpu.VMEM((layers, rows, width), BF16),
            pltpu.VMEM((layers, 2, hw, rows), BF16),
            pltpu.VMEM((layers, chips, 2, hw, rows), BF16),
            pltpu.VMEM((layers, chips, 2, hw, rows), BF16),
            pltpu.VMEM((layers, chips, 2, HEADS, rows), F32),
            pltpu.VMEM((layers, chips, 2, hw, rows), BF16),
            pltpu.VMEM((layers, chips, 2, HEADS, rows), F32),
            pltpu.VMEM((n_row, 2 * rows, hw), BF16),
            pltpu.VMEM((n_row, HALF, head_dim + 16, 2 * rows), BF16),
            pltpu.VMEM((chips, HALF, 2 * head_dim, 2 * rows), BF16),
            pltpu.VMEM((chips, HALF, head_dim + 16, 2 * rows), F32),
            pltpu.VMEM((chips, HEADS, 2 * rows), F32),
            dma((layers, n_row)),
            dma((layers, n_row)),
            dma((layers, n_row)),
            dma((layers, n_row)),
            dma((layers, chips, 2)),
            dma((layers, chips, 2)),
            dma((layers, chips, 2)),
            dma((layers, chips, 2)),
            dma((layers, chips, 2)),
            dma((layers, chips, 2)),
        ],
        compiler_params=pltpu.CompilerParams(
            collective_id=0, has_side_effects=True, vmem_limit_bytes=56 * 1024 * 1024
        ),
    )(node_feats, block_mask, w_qkv, w_out, w_up, w_down, ln_gain, ln_bias)


def solution(mesh):
    placed = (P(("row", "col"), None), P(), P(), P(), P(), P(), P(), P())
    body = functools.partial(per_device, mesh.shape["row"], mesh.shape["col"])
    return jax.shard_map(
        body, mesh=mesh, in_specs=placed, out_specs=P(("row", "col"), None), check_vma=False
    )
```
